32 devices in a mesh: seqs: 2 (over x), rows: 4 (over z), states: 4 (over y, core).
Axes of the slice: x: 2, y: 2, z: 4, core: 2. Of those that a mesh axis runs over, the one named last changes fastest.
Arguments:
- transition: bfloat16 [16384, 16384], P(None, ('rows', 'states'))
- emission: bfloat16 [16384, 10000], P(('rows', 'states'))
- init_probs: float32 [16384], P(('rows', 'states'))
- tokens: int32 [16, 48], P('seqs'), parts along dimension 0
- lengths: int32 [16], P('seqs'), parts along dimension 0
Outputs:
- output 1: float32 [16], P('seqs'), parts along dimension 0
- output 2: float32 [16, 16384], P('seqs', ('rows', 'states')), parts along dimension 0
There are 2 independent parts. The reference program is written for one: setup_inputs(seed, part) draws one part's arguments, and reference() takes and returns one part's arrays. A program takes and returns all parts, laid end to end along the dimension named above; an argument that names none is the same for every part.
All inputs are finite; a program needn't handle non-finite values.
Results may differ from the reference program's by a relative error of at most 0.0042.
Values are sent between devices in bfloat16 or wider.
A program may use at most 1 GiB of HBM per device.

```python
import math
import jax
import jax.numpy as jnp
from jax import lax

STATES = 16384
VOCAB_SIZE = 10000
SEQ_BATCH = 8
SEQ_STEPS = 48
ROW_BLOCK = min(STATES, 512)


def stochastic_rows(base_key, num_rows, num_cols, sigma):
    def one_block(block_idx):
        logits = sigma * jax.random.normal(jax.random.fold_in(base_key, block_idx), (ROW_BLOCK, num_cols), jnp.float32)
        return jax.nn.softmax(logits, axis=1).astype(jnp.bfloat16)
    blocks = lax.map(one_block, jnp.arange(num_rows // ROW_BLOCK))
    return blocks.reshape(num_rows, num_cols)


def setup_inputs(seed: int = 0, part: int = 0) -> dict:
    base_key = jax.random.key(seed)
    key_trans, key_emit, key_init = jax.random.split(base_key, 3)
    part_key = jax.random.fold_in(jax.random.key(seed + 1), part)
    key_tokens, key_lengths = jax.random.split(part_key)
    sigma_trans = math.sqrt(math.log(STATES / 8.0))
    sigma_emit = math.sqrt(math.log(VOCAB_SIZE / 32.0))
    transition = stochastic_rows(key_trans, STATES, STATES, sigma_trans)
    emission = stochastic_rows(key_emit, STATES, VOCAB_SIZE, sigma_emit)
    init_probs = jax.nn.softmax(sigma_trans * jax.random.normal(key_init, (STATES,), jnp.float32))
    tokens = jax.random.randint(key_tokens, (SEQ_BATCH, SEQ_STEPS), 0, VOCAB_SIZE, jnp.int32)
    lengths = jax.random.randint(key_lengths, (SEQ_BATCH,), 1, SEQ_STEPS + 1, jnp.int32)
    lengths = lengths.at[0].set(SEQ_STEPS)
    return dict(transition=transition, emission=emission, init_probs=init_probs, tokens=tokens, lengths=lengths)


def reference(transition, emission, init_probs, tokens, lengths):
    emit_first = jnp.take(emission, tokens[:, 0], axis=1).T
    alpha_init = init_probs[None, :] * emit_first
    first_norm = jnp.sum(alpha_init, axis=1)
    alpha_init = alpha_init / first_norm[:, None]
    log_init = jnp.log(first_norm)

    def step_fn(carry, step_inputs):
        alpha_prev, log_acc = carry
        tok_step, step_idx = step_inputs
        predicted = jnp.dot(alpha_prev.astype(jnp.bfloat16), transition, preferred_element_type=jnp.float32)
        alpha_new = predicted * jnp.take(emission, tok_step, axis=1).T
        step_norm = jnp.sum(alpha_new, axis=1)
        alpha_new = alpha_new / step_norm[:, None]
        alive_rows = step_idx < lengths
        alpha_next = jnp.where(alive_rows[:, None], alpha_new, alpha_prev)
        log_next = log_acc + jnp.where(alive_rows, jnp.log(step_norm), 0.0)
        return (alpha_next, log_next), None

    step_ids = jnp.arange(1, SEQ_STEPS, dtype=jnp.int32)
    final_state = lax.scan(step_fn, (alpha_init, log_init), (tokens.T[1:], step_ids))[0]
    alpha_last, loglik = final_state
    return loglik, alpha_last
```

```python
import functools
import jax
import jax.numpy as jnp
from jax import lax
from jax.experimental import pallas as pl
from jax.experimental.pallas import tpu as pltpu
from jax.sharding import PartitionSpec as P

STATE_AXES = ('rows', 'states')
ROWS, COLS = 4, 4
NUM_DEV = ROWS * COLS


def forward_kernel(trans_hbm, emit_ref, init_ref, len_ref, ll_ref, alpha_ref,
                   trans, gath, sums, load_sem, send_sem, csend_sem, recv_sem, crecv_sem):
    num_steps, batch, width = emit_ref.shape
    row = lax.axis_index('rows')
    col = lax.axis_index('states')

    def dev(r, s):
        return {'rows': r, 'states': s}

    r1 = row + 1 - 2 * lax.rem(row, 2)
    r2 = lax.rem(row + 2, 4)
    r3 = 3 - row
    sib = col + 1 - 2 * lax.rem(col, 2)
    opp = lax.rem(col + 2, 4)
    osib = opp + 1 - 2 * lax.rem(opp, 2)

    def blk(r, s):
        return r * COLS + s

    me = blk(row, col)

    load = pltpu.make_async_copy(trans_hbm, trans, load_sem)
    load.start()

    barrier = pltpu.get_barrier_semaphore()
    for d in range(1, NUM_DEV):
        peer = lax.rem(me + d, NUM_DEV)
        pl.semaphore_signal(barrier, inc=1, device_id=dev(peer // COLS, lax.rem(peer, COLS)),
                            device_id_type=pl.DeviceIdType.MESH)
    pl.semaphore_wait(barrier, NUM_DEV - 1)

    lane = lax.broadcasted_iota(jnp.int32, (batch, 128), 1)
    sub = lax.broadcasted_iota(jnp.int32, (batch, 128), 0)
    diag = lane == sub

    def send(p, k, slot, r, s):
        return pltpu.make_async_remote_copy(
            src_ref=gath.at[p, k], dst_ref=gath.at[p, k],
            send_sem=send_sem.at[slot], recv_sem=recv_sem.at[p, k],
            device_id=dev(r, s), device_id_type=pl.DeviceIdType.MESH)

    def csend(p, k, slot, r, s):
        return pltpu.make_async_remote_copy(
            src_ref=sums.at[p, k], dst_ref=sums.at[p, k],
            send_sem=csend_sem.at[slot], recv_sem=crecv_sem.at[p, k],
            device_id=dev(r, s), device_id_type=pl.DeviceIdType.MESH)

    def send_sums(p, a):
        total = jnp.sum(a, axis=1, keepdims=True)
        flat = jnp.sum(jnp.where(diag, total, 0.0), axis=0, keepdims=True)
        sums[p, me] = flat
        out = []
        for r in (r3, r2, r1, row):
            for s in (osib, opp, sib, col):
                if r is row and s is col:
                    continue
                c = csend(p, me, len(out), r, s)
                c.start()
                out.append(c)
        return out

    def wait_sums(p):
        for r in (row, r1, r2, r3):
            for s in (sib, opp, osib, col):
                if r is row and s is col:
                    continue
                csend(p, blk(r, s), 0, r, s).wait_recv()
        flat = jnp.sum(sums[p], axis=0)
        return jnp.sum(jnp.where(diag, jnp.broadcast_to(flat, (batch, 128)), 0.0), axis=1, keepdims=True)

    def update(t, a, c):
        alive = t < len_ref[...]
        alpha_ref[...] = jnp.where(alive[:, :1], a / c, alpha_ref[...])
        ll_ref[...] = ll_ref[...] + jnp.where(alive, jnp.log(jnp.broadcast_to(c, (batch, 128))), 0.0)

    ll_ref[...] = jnp.zeros_like(ll_ref)
    alpha_ref[...] = jnp.zeros_like(alpha_ref)

    def body(t, a):
        p = lax.rem(t, 2)
        gath[p, me] = a
        started = send_sums(p, a)
        slot = [0]

        def go(k, r, s):
            c = send(p, k, slot[0], r, s)
            slot[0] += 1
            c.start()
            started.append(c)

        def got(r, s):
            send(p, blk(r, s), 0, r, s).wait_recv()

        go(me, r3, col)
        go(me, r2, col)
        go(me, r1, col)
        go(me, row, opp)
        go(me, row, sib)
        got(row, opp)
        go(blk(row, opp), row, sib)
        for r in (r1, r2, r3):
            got(r, col)
            go(blk(r, col), row, opp)
            go(blk(r, col), row, sib)
        c = wait_sums(p)
        update(t, a, c)

        def part(r, s):
            k = blk(r, s)
            lhs = (gath[p, k] / c).astype(jnp.bfloat16)
            rhs = trans[pl.ds(pl.multiple_of(k * width, width), width), :]
            return jnp.dot(lhs, rhs, preferred_element_type=jnp.float32)

        u = part(row, col)
        u += part(row, opp)
        got(row, sib)
        u += part(row, sib)
        got(r1, opp)
        go(blk(r1, opp), row, sib)
        u += part(r1, col)
        u += part(r2, col)
        u += part(r3, col)
        got(r2, opp)
        go(blk(r2, opp), row, sib)
        u += part(r1, opp)
        got(r1, sib)
        got(row, osib)
        u += part(r1, sib)
        u += part(row, osib)
        got(r3, opp)
        go(blk(r3, opp), row, sib)
        got(r2, sib)
        got(r3, sib)
        u += part(r2, opp)
        u += part(r3, opp)
        u += part(r2, sib)
        u += part(r3, sib)
        got(r1, osib)
        u += part(r1, osib)
        got(r2, osib)
        u += part(r2, osib)
        got(r3, osib)
        u += part(r3, osib)
        for s in started:
            s.wait_send()
        return u * emit_ref[t + 1]

    first = init_ref[...] * emit_ref[0]
    load.wait()
    last = lax.fori_loop(0, num_steps - 1, body, first)
    p = (num_steps - 1) % 2
    started = send_sums(p, last)
    c = wait_sums(p)
    update(num_steps - 1, last, c)
    for s in started:
        s.wait_send()


def solution(mesh):
    def device_forward(transition_cols, emission_rows, init_probs, tokens, lengths):
        batch, num_steps = tokens.shape
        width, vocab = emission_rows.shape
        states = transition_cols.shape[0]
        picks = tokens.T.reshape(-1)
        onehot = (picks[:, None] == lax.broadcasted_iota(jnp.int32, (1, vocab), 1)).astype(jnp.bfloat16)
        emit = lax.dot_general(onehot, emission_rows, (((1,), (1,)), ((), ())),
                               preferred_element_type=jnp.float32)
        emit = emit.reshape(num_steps, batch, width)
        len_b = jnp.broadcast_to(lengths[:, None], (batch, 128))

        vmem = pl.BlockSpec(memory_space=pltpu.VMEM)
        ll, alpha = pl.pallas_call(
            forward_kernel,
            out_shape=(jax.ShapeDtypeStruct((batch, 128), jnp.float32),
                       jax.ShapeDtypeStruct((batch, width), jnp.float32)),
            in_specs=[pl.BlockSpec(memory_space=pl.ANY), vmem, vmem, vmem],
            out_specs=(vmem, vmem),
            scratch_shapes=[
                pltpu.VMEM((states, width), jnp.bfloat16),
                pltpu.VMEM((2, NUM_DEV, batch, width), jnp.float32),
                pltpu.VMEM((2, NUM_DEV, 1, 128), jnp.float32),
                pltpu.SemaphoreType.DMA,
                pltpu.SemaphoreType.DMA((16,)),
                pltpu.SemaphoreType.DMA((NUM_DEV,)),
                pltpu.SemaphoreType.DMA((2, NUM_DEV)),
                pltpu.SemaphoreType.DMA((2, NUM_DEV)),
            ],
            compiler_params=pltpu.CompilerParams(
                collective_id=0, has_side_effects=True, vmem_limit_bytes=56 * 1024 * 1024),
        )(transition_cols, emit, init_probs[None, :], len_b)
        return ll[:, 0], alpha

    return jax.shard_map(
        device_forward,
        mesh=mesh,
        in_specs=(P(None, STATE_AXES), P(STATE_AXES, None), P(STATE_AXES), P('seqs', None), P('seqs')),
        out_specs=(P('seqs'), P('seqs', STATE_AXES)),
        check_vma=False,
    )
```
